256 devices in a mesh: bank: 16 (over z, core), zero: 16 (over y, x).
Axes of the slice: x: 4, y: 4, z: 8, core: 2. Of those that a mesh axis runs over, the one named last changes fastest.
Arguments:
- master_gate: float32 [64, 2048, 1408], P('bank', 'zero'), may hold values from -0.1875 to 0.1875
- master_up: float32 [64, 2048, 1408], P('bank', 'zero'), may hold values from -0.1875 to 0.1875
- master_down: float32 [64, 1408, 2048], P('bank', None, 'zero'), may hold values from -0.21875 to 0.21875
- router_weight: float32 [2048, 64], P('zero', 'bank'), may hold values from -0.125 to 0.125
- router_gain: float32 [2048], P('zero'), may hold values from 0.25 to 1.75
Outputs:
- final_gate: bfloat16 [64, 2048, 1408], P('bank', None, 'zero')
- final_up: bfloat16 [64, 2048, 1408], P('bank', None, 'zero')
- final_down: bfloat16 [64, 1408, 2048], P('bank', 'zero')
- scale_gate: float32 [64, 1408], P('bank', 'zero')
- scale_up: float32 [64, 1408], P('bank', 'zero')
- scale_down: float32 [64, 1408], P('bank', 'zero')
- serve_router: bfloat16 [2048, 64], replicated
The draws below stay inside these ranges and needn't reach their ends.
All inputs are finite; a program needn't handle non-finite values. Where the reference program divides by a largest or mean magnitude, that divisor is 1e-20 or more.
Results may differ from the reference program's by a relative error of at most 0.0013.
Values may be sent and summed in bfloat16 or wider, within the bound.
No kernel may reach another device: no remote copies, remote signals or barrier semaphores. Data moves between devices by JAX's collectives and lax.ppermute only.
A program may use at most 64 MiB of HBM per device.

```python
import jax
import jax.numpy as jnp

EXPERTS = 64
D_MODEL = 2048
D_EXPERT = 1408


def strengthened(drawn, key, source, target, blocks, factor):
    owner, partner = [(jnp.arange(drawn.shape[axis_at]) // (drawn.shape[axis_at] // blocks)).reshape([-1 if axis == axis_at else 1 for axis in range(drawn.ndim)]) for axis_at in (source, target)]
    chosen = jax.random.permutation(key, blocks)[partner]
    strong = (owner == chosen) | (owner == (partner + blocks // 2) % blocks)
    return jnp.where(strong, factor * drawn, drawn)


def level_of(rng, extent, split, least, high):
    def one(position, parts):
        steps = jax.random.uniform(jax.random.fold_in(jax.random.fold_in(rng, 6), position), (parts,), jnp.float32, least / len(split), high / len(split))
        return jnp.repeat(jnp.exp(steps), extent[position] // parts).reshape((-1,) + (1,) * (len(extent) - position - 1))

    loudness = one(*split[0])
    for cut in split[1:]:
        loudness = loudness * one(*cut)
    return loudness


def normal_values(own_key, dims, width, reach, cuts=(), held_as=jnp.bfloat16):
    values = width * jax.random.normal(own_key, dims, jnp.float32)
    if cuts:
        values = values * level_of(own_key, dims, cuts, -0.22, 0.18)
    return jnp.clip(values, -reach, reach).astype(held_as)


def noise_with(own_key, extent, scale, reach, pieces, heavy, dtype=jnp.bfloat16):
    entries = scale * jax.random.normal(own_key, extent, jnp.float32)
    if pieces:
        entries = entries * level_of(own_key, extent, pieces, -0.22, 0.18)
    return jnp.clip(strengthened(entries, jax.random.fold_in(own_key, 3), *heavy), -reach, reach).astype(dtype)


def setup_inputs(seed: int = 0) -> dict:
    keys = jax.random.split(jax.random.key(seed), 6)
    return {
        "master_gate": noise_with(keys[0], (EXPERTS, D_MODEL, D_EXPERT), D_MODEL ** -0.5, 0.1875, ((0, 16), (1, 16)), (1, 2, 16, 2.0), jnp.float32),
        "master_up": noise_with(keys[1], (EXPERTS, D_MODEL, D_EXPERT), D_MODEL ** -0.5, 0.1875, ((0, 16), (1, 16)), (1, 2, 16, 2.0), jnp.float32),
        "master_down": noise_with(keys[2], (EXPERTS, D_EXPERT, D_MODEL), D_EXPERT ** -0.5, 0.21875, ((0, 16), (2, 16)), (2, 1, 16, 2.0), jnp.float32),
        "router_weight": normal_values(keys[3], (D_MODEL, EXPERTS), D_MODEL ** -0.5, 0.125, ((0, 16), (1, 16)), jnp.float32),
        "router_gain": jnp.clip(1.0 + 0.15 * jax.random.normal(keys[4], (D_MODEL,), jnp.float32), 0.25, 1.75),
    }


def reference(master_gate, master_up, master_down, router_weight, router_gain):
    scale_gate = jnp.sum(jnp.abs(master_gate), axis=1) / D_MODEL
    final_gate = (master_gate / jnp.expand_dims(scale_gate, 1)).astype(jnp.bfloat16)
    scale_up = jnp.sum(jnp.abs(master_up), axis=1) / D_MODEL
    final_up = (master_up / jnp.expand_dims(scale_up, 1)).astype(jnp.bfloat16)
    scale_down = jnp.sum(jnp.abs(master_down), axis=2) / D_MODEL
    final_down = (master_down / jnp.expand_dims(scale_down, 2)).astype(jnp.bfloat16)
    serve_router = (router_weight * router_gain[:, None]).astype(jnp.bfloat16)
    return final_gate, final_up, final_down, scale_gate, scale_up, scale_down, serve_router
```

```python
import jax
import jax.numpy as jnp
from jax import lax
from jax.experimental import pallas as pl
from jax.experimental.pallas import tpu as pltpu
from jax.sharding import PartitionSpec as P

D_MODEL = 2048
LANES = 128
TINY = 1e-25
REACH = 2.0**0.9


def coded(v):
    for _ in range(4):
        v = v * jnp.abs(v)
    return v


def decoded(y):
    a = jnp.abs(y)
    r = jnp.exp(jnp.log(jnp.maximum(a, 1e-38)) * (1 / 16))
    return jnp.where(y > 0, r, jnp.where(y < 0, -r, 0.0))


def in_two(p):
    high = p.astype(jnp.bfloat16).astype(jnp.float32)
    low = (p - high).astype(jnp.bfloat16).astype(jnp.float32)
    return high, low


def normaliser(p):
    return (LANES * REACH) / jnp.maximum(p, TINY)


def encode_body(gate, up, down, out, sums, cols, *, groups, rows, experts):
    k = pl.program_id(0)
    across = lax.broadcasted_iota(jnp.int32, (rows, LANES), 1)

    def turned(x):
        p = jnp.sum(jnp.abs(x), axis=0, keepdims=True)
        high, low = in_two(p)
        y = coded(x * normaliser(high + low))
        yt = y.T
        for d in range(groups):
            out[d] = yt[d * rows : (d + 1) * rows].astype(jnp.bfloat16)
        sums[pl.ds(2 * k, 1)] = high
        sums[pl.ds(2 * k + 1, 1)] = low

    @pl.when(k < experts)
    def _():
        turned(gate[0])

    @pl.when((k >= experts) & (k < 2 * experts))
    def _():
        turned(up[0])

    @pl.when((k >= 2 * experts) & (k < 3 * experts))
    def _():
        e = k - 2 * experts
        for d in range(groups):
            x = down[0, d * rows : (d + 1) * rows]
            p = jnp.sum(jnp.abs(x), axis=1, keepdims=True)
            high, low = in_two(p)
            out[d] = coded(x * normaliser(high + low)).astype(jnp.bfloat16)
            both = jnp.where(across == 2 * e, high, jnp.where(across == 2 * e + 1, low, 0.0))
            cols[d] = jnp.where(e == 0, both, cols[d] + both)

    @pl.when(k == 3 * experts)
    def _():
        for d in range(groups):
            turned_sums = sums[:, d * rows : (d + 1) * rows]
            down_sums = cols[d].T[: 2 * experts]
            both = jnp.concatenate([turned_sums, down_sums], axis=0)
            both = jnp.pad(both, ((0, 0), (0, LANES - rows)))
            out[d, : 6 * experts] = both.astype(jnp.bfloat16)


def encode(gate, up, down, groups):
    experts, part, inner = gate.shape
    rows = inner // groups
    total = 3 * experts * rows + 6 * experts

    def block(first):
        return lambda k: (jnp.clip(k - first, 0, experts - 1), 0, 0)

    def body(*refs):
        encode_body(*refs, groups=groups, rows=rows, experts=experts)

    return pl.pallas_call(
        body,
        grid=(3 * experts + 1,),
        in_specs=[
            pl.BlockSpec((1, part, inner), block(0)),
            pl.BlockSpec((1, part, inner), block(experts)),
            pl.BlockSpec((1, inner, part), block(2 * experts)),
        ],
        out_specs=pl.BlockSpec((groups, rows, LANES), lambda k: (0, k, 0)),
        out_shape=jax.ShapeDtypeStruct((groups, total, LANES), jnp.bfloat16),
        scratch_shapes=[
            pltpu.VMEM((4 * experts, inner), jnp.float32),
            pltpu.VMEM((groups, rows, LANES), jnp.float32),
        ],
        name="encode",
    )(gate, up, down)


def decode_body(data, sums, gate, up, down, scales, factor, *, groups, rows, experts):
    k = pl.program_id(0)
    n = 3 * experts

    @pl.when(k == 0)
    def _():
        own = []
        for s in range(groups):
            words = sums[s].astype(jnp.float32)
            own.append(words.reshape(n, 2, LANES).sum(axis=1))
        scale = sum(own) / D_MODEL
        scales[...] = scale
        scale = jnp.where(scale > 0, scale, 1.0)
        for s in range(groups):
            f = jnp.maximum(own[s], TINY) / (LANES * REACH) / scale
            f = jnp.pad(f, ((0, LANES - n), (0, 0)))
            factor[s] = f.T

    column = lax.broadcasted_iota(jnp.int32, (LANES, LANES), 1)
    for s in range(groups):
        f = jnp.sum(jnp.where(column == k, factor[s], 0.0), axis=1, keepdims=True)[:rows]
        y = (decoded(data[s].astype(jnp.float32)) * f).astype(jnp.bfloat16)
        at = slice(s * LANES, (s + 1) * LANES)

        @pl.when(k < experts)
        def _():
            gate[0, :, at] = y

        @pl.when((k >= experts) & (k < 2 * experts))
        def _():
            up[0, :, at] = y

        @pl.when(k >= 2 * experts)
        def _():
            down[0, :, at] = y


def decode(received, experts, rows):
    groups = received.shape[0]
    n = 3 * experts

    def block(first):
        return lambda k: (jnp.clip(k - first, 0, experts - 1), 0, 0)

    def body(*refs):
        decode_body(*refs, groups=groups, rows=rows, experts=experts)

    final = jax.ShapeDtypeStruct((experts, rows, groups * LANES), jnp.bfloat16)
    return pl.pallas_call(
        body,
        grid=(n,),
        in_specs=[
            pl.BlockSpec((groups, rows, LANES), lambda k: (0, k, 0)),
            pl.BlockSpec((groups, 2 * n, LANES), lambda k: (0, n * rows // (2 * n), 0)),
        ],
        out_specs=[
            pl.BlockSpec((1, rows, groups * LANES), block(0)),
            pl.BlockSpec((1, rows, groups * LANES), block(experts)),
            pl.BlockSpec((1, rows, groups * LANES), block(2 * experts)),
            pl.BlockSpec((n, LANES), lambda k: (0, 0)),
        ],
        out_shape=[final, final, final, jax.ShapeDtypeStruct((n, LANES), jnp.float32)],
        scratch_shapes=[pltpu.VMEM((groups, LANES, LANES), jnp.float32)],
        name="decode",
    )(received, received)


def local(master_gate, master_up, master_down, router_weight, router_gain):
    groups = lax.axis_size("zero")
    experts, _, inner = master_gate.shape
    rows = inner // groups
    sent = encode(master_gate, master_up, master_down, groups)
    received = lax.all_to_all(sent, "zero", 0, 0, tiled=True)
    gate, up, down, scales = decode(received, experts, rows)
    part = (router_weight * router_gain[:, None]).astype(jnp.bfloat16).T
    row = lax.all_gather(part, "zero", axis=1, tiled=True)
    router = lax.all_gather(row, "bank", axis=0, tiled=True)
    scale = scales[:, :rows]
    return (
        jnp.swapaxes(gate, 1, 2),
        jnp.swapaxes(up, 1, 2),
        down,
        scale[:experts],
        scale[experts : 2 * experts],
        scale[2 * experts :],
        router.T,
    )


def solution(mesh):
    placed = (
        P("bank", "zero", None),
        P("bank", "zero", None),
        P("bank", None, "zero"),
        P("zero", "bank"),
        P("zero"),
    )
    return jax.shard_map(
        local,
        mesh=mesh,
        in_specs=placed,
        out_specs=(
            P("bank", None, "zero"),
            P("bank", None, "zero"),
            P("bank", "zero", None),
            P("bank", "zero"),
            P("bank", "zero"),
            P("bank", "zero"),
            P(),
        ),
        check_vma=False,
    )
```

```python
import jax
import jax.numpy as jnp
from jax import lax
from jax.experimental import pallas as pl
from jax.experimental.pallas import tpu as pltpu
from jax.sharding import PartitionSpec as P

D_MODEL = 2048
LANES = 128
POWER = 15
TINY = 1e-25
REACH = LANES * 2.0**1.5
ACROSS = (((1,), (1,)), ((), ()))
SIDE = 4
SHIFTS = (
    (0, 1), (0, 3), (1, 0), (3, 0), (1, 1), (3, 3), (1, 3), (3, 1),
    (0, 2), (2, 0), (1, 2), (2, 1), (3, 2), (2, 3), (2, 2),
)


def partner(i, shift, sign):
    y = (i // SIDE + sign * shift[0]) % SIDE
    return y * SIDE + (i % SIDE + sign * shift[1]) % SIDE


def partners(me, sign):
    low = SIDE - 1
    found = [me]
    for dy, dx in SHIFTS:
        y = (me + SIDE * ((sign * dy) & low)) & (SIDE * low)
        found.append(y | ((me + ((sign * dx) & low)) & low))
    return found


def coded(v):
    cube = v * v * v
    sixth = cube * cube
    return (sixth * sixth * cube).astype(jnp.bfloat16)


def restored(y, factor):
    size = jnp.maximum(jnp.abs(y), 1e-37)
    return y * jnp.exp2(jnp.log2(size) * (1 / POWER - 1)) * factor


def in_two(p):
    high = p.astype(jnp.bfloat16).astype(jnp.float32)
    low = (p - high).astype(jnp.bfloat16).astype(jnp.float32)
    return high, low


def own_sums(x, axis):
    high, low = in_two(jnp.sum(jnp.abs(x), axis=axis, keepdims=True))
    return high, low, REACH / jnp.maximum(high + low, TINY)


def identity(rows):
    shape = (rows, LANES)
    eye = lax.broadcasted_iota(jnp.int32, shape, 0) == lax.broadcasted_iota(jnp.int32, shape, 1)
    return eye.astype(jnp.float32).astype(jnp.bfloat16)


def encode_body(me, *refs, groups, rows, experts):
    given, outs = refs[:3], refs[3 : 3 + groups]
    held = refs[3 + groups : 6 + groups]
    stage, turned, sums, cols, arrived, left = refs[6 + groups :]
    inner = groups * rows
    part = experts * rows
    dest = [pl.multiple_of(d * rows, 8) for d in partners(me[0], 1)]

    def fetch(a, e):
        return pltpu.make_async_copy(given[a].at[e], held[a].at[e], arrived.at[a, e])

    def send(t, first, last):
        at = pl.ds(first, last - first)
        pltpu.make_async_copy(stage.at[t, at], outs[t].at[at], left.at[t]).start()

    for a in range(3):
        for e in range(experts):
            fetch(a, e).start()

    def turn(a):
        def one(e, _):
            fetch(a, e).wait()
            x = held[a][e]
            high, low, norm = own_sums(x, 0)
            y = coded(x * norm)
            eye = identity(LANES)
            for b in range(inner // LANES):
                at = slice(b * LANES, (b + 1) * LANES)
                turned[at] = lax.dot_general(eye, y[:, at], ACROSS, preferred_element_type=jnp.float32)
            k = a * experts + e
            for t in range(groups):
                at = pl.ds(pl.multiple_of(k * rows, 8), rows)
                stage[t, at] = turned[pl.ds(dest[t], rows)].astype(jnp.bfloat16)
            sums[pl.ds(k, 1)] = high
            sums[pl.ds(2 * experts + k, 1)] = low
            return 0

        lax.fori_loop(0, experts, one, 0)
        for t in range(groups):
            send(t, a * part, (a + 1) * part)

    turn(0)
    turn(1)
    lane = lax.broadcasted_iota(jnp.int32, (rows, LANES), 1)

    def keep(e, _):
        fetch(2, e).wait()
        for t in range(groups):
            x = held[2][e, pl.ds(dest[t], rows)]
            high, low, norm = own_sums(x, 1)
            at = pl.ds(pl.multiple_of((2 * experts + e) * rows, 8), rows)
            stage[t, at] = coded(x * norm)
            cols[t] = jnp.where(lane == e, high, jnp.where(lane == experts + e, low, cols[t]))
        return 0

    lax.fori_loop(0, experts, keep, 0)
    n = 2 * experts
    for d in range(groups):
        some = sums[:, d * rows : (d + 1) * rows]
        turned[d * rows : d * rows + 2 * n] = jnp.pad(some, ((0, 0), (0, LANES - rows)))
    for t in range(groups):
        own = jnp.where(lane < n, cols[t], 0.0).astype(jnp.bfloat16)
        own = lax.dot_general(identity(n), own, ACROSS, preferred_element_type=jnp.float32)
        own = jnp.pad(own, ((0, 0), (0, LANES - rows)))
        both = jnp.concatenate([turned[pl.ds(dest[t], 2 * n)], own], axis=0)
        stage[t, 3 * part :] = both.astype(jnp.bfloat16)
        send(t, 2 * part, 3 * part + 3 * n)
    for t in range(groups):
        pltpu.make_async_copy(stage.at[t], outs[t], left.at[t]).wait()


def encode(gate, up, down, me, groups):
    experts, _, inner = gate.shape
    rows = inner // groups
    total = 3 * experts * rows + 6 * experts

    def body(*refs):
        encode_body(*refs, groups=groups, rows=rows, experts=experts)

    anywhere = pl.BlockSpec(memory_space=pl.ANY)
    return pl.pallas_call(
        body,
        in_specs=[pl.BlockSpec(memory_space=pltpu.SMEM)] + [anywhere] * 3,
        out_specs=[anywhere] * groups,
        out_shape=[jax.ShapeDtypeStruct((total, LANES), jnp.bfloat16)] * groups,
        scratch_shapes=[
            pltpu.VMEM(gate.shape, jnp.float32),
            pltpu.VMEM(up.shape, jnp.float32),
            pltpu.VMEM(down.shape, jnp.float32),
            pltpu.VMEM((groups, total, LANES), jnp.bfloat16),
            pltpu.VMEM((inner, LANES), jnp.float32),
            pltpu.VMEM((4 * experts, inner), jnp.float32),
            pltpu.VMEM((groups, rows, LANES), jnp.float32),
            pltpu.SemaphoreType.DMA((3, experts)),
            pltpu.SemaphoreType.DMA((groups,)),
        ],
        name="encode",
    )(me, gate, up, down)


def decode_body(me, *refs, groups, rows, experts):
    data, outs = refs[:groups], refs[groups : groups + 3]
    scales, stage, factor, left = refs[groups + 3 :]
    source = [pl.multiple_of(d * LANES, LANES) for d in partners(me[0], -1)]
    n = 3 * experts
    m = 2 * experts
    own = []
    for g in range(groups):
        words = data[g][n * rows :].astype(jnp.float32)
        turned = words[:m] + words[m : 2 * m]
        kept = words[2 * m : 2 * m + experts] + words[2 * m + experts :]
        own.append((turned, kept))
    for first, size, parts in ((0, m, [o[0] for o in own]), (m, experts, [o[1] for o in own])):
        scale = sum(parts) / D_MODEL
        scales[first : first + size] = scale
        scale = 1 / (REACH * jnp.where(scale > 0, scale, 1.0))
        for g in range(groups):
            factor[first : first + size, g] = jnp.maximum(parts[g], TINY) * scale

    def copy(a, e):
        return pltpu.make_async_copy(stage.at[a, e], outs[a].at[e], left.at[a, e])

    for a in range(3):

        def one(e, _, a=a):
            k = a * experts + e
            f = factor[k].T
            for g in range(groups):
                y = data[g][pl.ds(pl.multiple_of(k * rows, 8), rows)].astype(jnp.float32)
                y = restored(y, f[:rows, g : g + 1])
                stage[a, e, :, pl.ds(source[g], LANES)] = y.astype(jnp.bfloat16)
            copy(a, e).start()
            return 0

        lax.fori_loop(0, experts, one, 0)
    for a in range(3):
        for e in range(experts):
            copy(a, e).wait()


def decode(pieces, me, experts, rows):
    groups = len(pieces)
    n = 3 * experts

    def body(*refs):
        decode_body(*refs, groups=groups, rows=rows, experts=experts)

    final = jax.ShapeDtypeStruct((experts, rows, groups * LANES), jnp.bfloat16)
    anywhere = pl.BlockSpec(memory_space=pl.ANY)
    here = pl.BlockSpec(memory_space=pltpu.VMEM)
    return pl.pallas_call(
        body,
        in_specs=[pl.BlockSpec(memory_space=pltpu.SMEM)] + [here] * groups,
        out_specs=[anywhere, anywhere, anywhere, here],
        out_shape=[final, final, final, jax.ShapeDtypeStruct((n, LANES), jnp.float32)],
        scratch_shapes=[
            pltpu.VMEM((3, experts, rows, groups * LANES), jnp.bfloat16),
            pltpu.VMEM((n, groups, LANES), jnp.float32),
            pltpu.SemaphoreType.DMA((3, experts)),
        ],
        compiler_params=pltpu.CompilerParams(vmem_limit_bytes=10 << 20),
        name="decode",
    )(me, *pieces)


def rolled(parts, by):
    rows = sum(p.shape[0] for p in parts)

    def body(by, *refs):
        x = jnp.concatenate([r[...].astype(jnp.float32) for r in refs[:-1]], axis=0)
        refs[-1][...] = pltpu.roll(x, by[0], 0).astype(jnp.bfloat16)

    return pl.pallas_call(
        body,
        in_specs=[pl.BlockSpec(memory_space=pltpu.SMEM)]
        + [pl.BlockSpec(memory_space=pltpu.VMEM)] * len(parts),
        out_specs=pl.BlockSpec(memory_space=pltpu.VMEM),
        out_shape=jax.ShapeDtypeStruct((rows, parts[0].shape[1]), jnp.bfloat16),
        compiler_params=pltpu.CompilerParams(vmem_limit_bytes=4 << 20),
        name="rolled",
    )(by, *parts)


def gathered(x, axis):
    count, n = lax.axis_size(axis), 1
    rows, parts = x.shape[0], [x]
    while n < count:
        perm = [((i + n) % count, i) for i in range(count)]
        parts.append(lax.ppermute(jnp.concatenate(parts, axis=0), axis, perm))
        n *= 2
    return rolled(parts, (lax.axis_index(axis) * rows).astype(jnp.int32).reshape(1))


def local(master_gate, master_up, master_down, router_weight, router_gain):
    groups = lax.axis_size("zero")
    experts, _, inner = master_gate.shape
    rows = inner // groups
    me = lax.axis_index("zero").astype(jnp.int32).reshape(1)
    sent = encode(master_gate, master_up, master_down, me, groups)
    pieces = [sent[0]]
    for t, s in enumerate(SHIFTS):
        perm = [(i, partner(i, s, 1)) for i in range(groups)]
        pieces.append(lax.ppermute(sent[t + 1], "zero", perm))
    gate, up, down, scales = decode(pieces, me, experts, rows)
    part = (router_weight * router_gain[:, None]).astype(jnp.bfloat16).T
    copies = jnp.broadcast_to(part[None], (groups, *part.shape))
    row = lax.all_to_all(copies, "zero", 0, 0, tiled=True)
    row = jnp.swapaxes(row, 0, 1).reshape(part.shape[0], -1)
    router = gathered(row, "bank")
    scale = scales[:, :rows]
    return (
        jnp.swapaxes(gate, 1, 2),
        jnp.swapaxes(up, 1, 2),
        down,
        scale[:experts],
        scale[experts : 2 * experts],
        scale[2 * experts :],
        router.T,
    )


def solution(mesh):
    placed = (
        P("bank", "zero", None),
        P("bank", "zero", None),
        P("bank", None, "zero"),
        P("zero", "bank"),
        P("zero"),
    )
    return jax.shard_map(
        local,
        mesh=mesh,
        in_specs=placed,
        out_specs=(
            P("bank", None, "zero"),
            P("bank", None, "zero"),
            P("bank", "zero", None),
            P("bank", "zero"),
            P("bank", "zero"),
            P("bank", "zero"),
            P(),
        ),
        check_vma=False,
    )
```
